256 devices in a mesh: batch: 16 (over z_hi, y), ctx: 16 (over z_lo, x, core).
Axes of the slice: x: 4, y: 4, z: 8 (z_hi: 4, z_lo: 2; z = z_hi * 2 + z_lo), core: 2. Of those that a mesh axis runs over, the one named last changes fastest.
Arguments:
- asked_for: bfloat16 [32, 4096, 16, 128], P('batch', 'ctx'), may hold values from -6 to 6
- offered: bfloat16 [32, 4096, 16, 128], P('batch', 'ctx'), may hold values from -6 to 6
- contents: bfloat16 [32, 4096, 16, 128], P('batch', 'ctx'), may hold values from -6 to 6
- gate_rows: bfloat16 [32, 4096, 16, 128], P('batch', 'ctx'), may hold values from -6 to 6
- out_weight: bfloat16 [2048, 2048], P('batch'), may hold values from -0.125 to 0.125
Outputs:
- block_out: bfloat16 [32, 4096, 2048], P('batch', 'ctx')
The draws below stay inside these ranges and needn't reach their ends.
All inputs are finite; a program needn't handle non-finite values.
Results may differ from the reference program's by a relative error of at most 0.006.
Values may be sent and summed in bfloat16 or wider, within the bound.
No kernel may reach another device: no remote copies, remote signals or barrier semaphores. Data moves between devices by JAX's collectives and lax.ppermute only.
A program may use at most 128 MiB of HBM per device.

```python
import jax
import jax.numpy as jnp
from jax import lax

HEADS = 16
HEAD_SIZE = 128
BATCH = 32
TOKENS = 4096
WIDTH = 2048


def shard_levels(key, shape, shards, low, high):
    def one(dim, parts):
        heights = jax.random.uniform(jax.random.fold_in(jax.random.fold_in(key, 6), dim), (parts,), jnp.float32, low / len(shards), high / len(shards))
        return jnp.repeat(jnp.exp(heights), shape[dim] // parts).reshape((-1,) + (1,) * (len(shape) - dim - 1))

    factor_of = one(*shards[0])
    for cut in shards[1:]:
        factor_of = factor_of * one(*cut)
    return factor_of


def normal_values(rng, extent, deviation, limit, split=(), dtype=jnp.bfloat16):
    values = deviation * jax.random.normal(rng, extent, jnp.float32)
    if split:
        values = values * shard_levels(rng, extent, split, -0.22, 0.18)
    return jnp.clip(values, -limit, limit).astype(dtype)


def setup_inputs(seed: int = 0) -> dict:
    key_of = jax.random.split(jax.random.key(seed), 6)
    asked_for = normal_values(key_of[0], (BATCH, TOKENS, HEADS, HEAD_SIZE), 1.0, 6.0, ((0, 16), (1, 16)))
    offered = normal_values(key_of[1], (BATCH, TOKENS, HEADS, HEAD_SIZE), 1.0, 6.0, ((0, 16), (1, 16)))
    contents = normal_values(key_of[2], (BATCH, TOKENS, HEADS, HEAD_SIZE), 1.0, 6.0, ((0, 16), (1, 16)))
    gate_rows = normal_values(key_of[3], (BATCH, TOKENS, HEADS, HEAD_SIZE), 1.0, 6.0, ((0, 16), (1, 16)))
    out_weight = normal_values(key_of[4], (WIDTH, WIDTH), WIDTH ** -0.5, 0.125, ((0, 16),))
    return {"asked_for": asked_for, "offered": offered, "contents": contents, "gate_rows": gate_rows, "out_weight": out_weight}


def to_features(values):
    wide = values.astype(jnp.float32)
    return (jnp.where(wide > 0.0, wide + 1.0, jnp.exp(jnp.minimum(wide, 0.0)))).astype(jnp.bfloat16)


def close_heads(read, gate_rows, count):
    result = read * count ** 0.5
    result = result * jax.nn.sigmoid(gate_rows.astype(jnp.float32))
    return result.astype(jnp.bfloat16)


def ask_state(features, state, mass):
    small = lax.optimization_barrier(state.astype(jnp.bfloat16))
    top = jnp.einsum("bthd,bhde->bthe", features.astype(jnp.float32), small.astype(jnp.float32))
    bottom = jnp.einsum("bthd,bhd->bth", features.astype(jnp.float32), mass, precision=lax.Precision.HIGHEST)
    return top / (bottom + 1e-3)[..., None]


def reference(asked_for, offered, contents, gate_rows, out_weight):
    query_feature, key_feature = lax.optimization_barrier((to_features(asked_for), to_features(offered)))
    state = jnp.einsum("bthd,bthe->bhde", key_feature.astype(jnp.float32), contents.astype(jnp.float32)) / TOKENS
    mass = jnp.sum(key_feature.astype(jnp.float32), axis=1) / TOKENS
    mixed = close_heads(ask_state(query_feature, state, mass), gate_rows, TOKENS).reshape(BATCH, TOKENS, WIDTH)
    mixed = lax.optimization_barrier(mixed)
    block_out = jnp.einsum("btw,wv->btv", mixed.astype(jnp.float32), out_weight.astype(jnp.float32)).astype(jnp.bfloat16)
    return block_out
```

```python
import jax
import jax.numpy as jnp
from jax import lax
from jax.experimental import pallas as pl
from jax.experimental.pallas import tpu as pltpu
from jax.sharding import Mesh
from jax.sharding import PartitionSpec as P

BATCH = ("zh", "y")
CTX = ("zl", "x", "core")
HEADS, SIZE, WIDTH = 16, 128, 2048
HALF = 1024
XC = 512
YC = HALF - XC


def from_offset(value, axis, step, n=4):
    return lax.ppermute(value, axis, [((k + step) % n, k) for k in range(n)])


def gathered(value, axis):
    return [value] + [from_offset(value, axis, i) for i in (1, 3, 2)]


OFFS = (0, 1, 3, 2)


def swapped(value):
    return lax.ppermute(value, "core", [(0, 1), (1, 0)])


def to_features(values):
    wide = values.astype(jnp.float32)
    return jnp.where(wide > 0.0, wide + 1.0, jnp.exp(jnp.minimum(wide, 0.0))).astype(jnp.bfloat16)


def gather_weight(weight):
    core, x = lax.axis_index("core"), lax.axis_index("x")
    mine_y = lax.dynamic_slice(weight, (0, core * HALF + XC), (128, YC))
    mine_x = lax.dynamic_slice(weight, (x * 32, core * HALF), (32, XC))
    by_z_y = jnp.stack(gathered(mine_y, "zh"))
    by_z_x = jnp.stack(gathered(mine_x, "zh"))
    y_parts = gathered(by_z_y, "y")
    x_parts = gathered(jnp.stack(gathered(by_z_x, "y")), "x")
    return y_parts + x_parts


def project_kernel(where, mixed_ref, *rest):
    chunks, (out_ref, held, sems) = rest[:16], rest[16:]
    zh, y, x, core = where[0], where[1], where[2], where[3]
    copies = ([], [])
    for k in range(2):
        base = (core if k == 0 else 1 - core) * HALF
        for j in range(4):
            for z in range(4):
                row = (lax.rem(zh + OFFS[z], 4) * 4 + lax.rem(y + OFFS[j], 4)) * 128
                copies[k].append(
                    pltpu.make_async_copy(
                        chunks[k * 8 + j].at[z],
                        held.at[
                            pl.ds(pl.multiple_of(row, 128), 128),
                            pl.ds(pl.multiple_of(base + XC, 128), YC),
                        ],
                        sems.at[k],
                    )
                )
                for i in range(4):
                    start = row + lax.rem(x + OFFS[i], 4) * 32
                    copies[k].append(
                        pltpu.make_async_copy(
                            chunks[k * 8 + 4 + i].at[j, z],
                            held.at[
                                pl.ds(pl.multiple_of(start, 32), 32),
                                pl.ds(pl.multiple_of(base, 128), XC),
                            ],
                            sems.at[k],
                        )
                    )
    for k in range(2):
        for copy in copies[k]:
            copy.start()
    for k in range(2):
        base = (core if k == 0 else 1 - core) * HALF
        for copy in copies[k]:
            copy.wait()
        for n in range(2):
            cols = pl.ds(pl.multiple_of(base + n * 512, 512), 512)
            out_ref[:, cols] = jnp.dot(
                mixed_ref[...], held[:, cols], preferred_element_type=jnp.float32
            ).astype(jnp.bfloat16)


def project(where, mixed, chunks):
    return pl.pallas_call(
        project_kernel,
        out_shape=jax.ShapeDtypeStruct((512, WIDTH), jnp.bfloat16),
        in_specs=[
            pl.BlockSpec(memory_space=pltpu.SMEM),
            pl.BlockSpec(memory_space=pltpu.VMEM),
        ]
        + [pl.BlockSpec(memory_space=pltpu.HBM)] * 16,
        out_specs=pl.BlockSpec(memory_space=pltpu.VMEM),
        scratch_shapes=[pltpu.VMEM((WIDTH, WIDTH), jnp.bfloat16), pltpu.SemaphoreType.DMA((2,))],
        cost_estimate=pl.CostEstimate(
            flops=2 * 512 * WIDTH * WIDTH, bytes_accessed=12 << 20, transcendentals=0
        ),
        compiler_params=pltpu.CompilerParams(vmem_limit_bytes=32 << 20),
    )(where, mixed, *chunks)


def add_up(parts):
    return sum(part.astype(jnp.float32) for part in parts)


def reduce_state(payload):
    core, x = lax.axis_index("core"), lax.axis_index("x")
    halves = payload.reshape(2, 8, 2, 144, SIZE)
    keep = lax.dynamic_index_in_dim(halves, core, 0, keepdims=False)
    give = lax.dynamic_index_in_dim(halves, 1 - core, 0, keepdims=False)
    mine = add_up((keep, swapped(give))).astype(jnp.bfloat16).reshape(4, 2, 2, 144, SIZE)
    parts = [lax.dynamic_index_in_dim(mine, x, 0, keepdims=False)]
    for i in (1, 3, 2):
        part = lax.dynamic_index_in_dim(mine, lax.rem(x + 4 - i, 4), 0, keepdims=False)
        parts.append(from_offset(part, "x", i))
    two = add_up(parts).astype(jnp.bfloat16)
    two = add_up((two, lax.ppermute(two, "zl", [(0, 1), (1, 0)]))).astype(jnp.bfloat16)
    pieces = gathered(two, "x")
    half = jnp.stack([pieces[0], pieces[1], pieces[3], pieces[2]])
    both = jnp.stack([half, swapped(half)])
    both = jnp.concatenate([both, both], 1)
    both = lax.dynamic_slice_in_dim(both, lax.rem(4 - x, 4), 4, 1)
    both = jnp.where(core == 0, both, both[::-1])
    return both.reshape(16, 2, 144, SIZE)


def local(asked_for, offered, contents, gate_rows, out_weight):
    chunks = gather_weight(out_weight)
    chunks = chunks + [swapped(chunk) for chunk in chunks]
    key_feature = to_features(offered)
    part_state = jnp.einsum(
        "bthd,bthe->hbde", key_feature, contents, preferred_element_type=jnp.float32
    )
    part_mass = jnp.sum(key_feature.astype(jnp.float32), axis=1).transpose(1, 0, 2)
    payload = jnp.concatenate(
        [part_state, jnp.broadcast_to(part_mass[:, :, None], (16, 2, 16, SIZE))], 2
    ).astype(jnp.bfloat16)
    total = reduce_state(payload)
    query_feature = to_features(asked_for)
    top = jnp.einsum(
        "bthd,hbde->bthe", query_feature, total[:, :, :SIZE], preferred_element_type=jnp.float32
    )
    bottom = jnp.einsum(
        "bthd,hbd->bth", query_feature, total[:, :, SIZE], preferred_element_type=jnp.float32
    )
    result = top / (bottom + 4.096)[..., None] * 64.0
    result = result * jax.nn.sigmoid(gate_rows.astype(jnp.float32))
    mixed = result.astype(jnp.bfloat16).reshape(512, WIDTH)
    where = jnp.stack([lax.axis_index(a) for a in ("zh", "y", "x", "core")]).astype(jnp.int32)
    return project(where, mixed, chunks).reshape(2, 256, WIDTH)


def solution(mesh):
    finer = Mesh(mesh.devices.reshape(4, 4, 2, 4, 2), BATCH + CTX)
    rows = P(BATCH, CTX, None, None)
    return jax.shard_map(
        local,
        mesh=finer,
        in_specs=(rows, rows, rows, rows, P(BATCH, None)),
        out_specs=P(BATCH, CTX, None),
        check_vma=False,
    )
```

```python
import jax
import jax.numpy as jnp
from jax import lax
from jax.experimental import pallas as pl
from jax.experimental.pallas import tpu as pltpu
from jax.sharding import Mesh
from jax.sharding import PartitionSpec as P

BATCH = ("zh", "y")
CTX = ("zl", "x", "core")
HEADS, SIZE, WIDTH = 16, 128, 2048
HALF = 1024
NX = 2
NY = 4 - NX
BLOCKS = ((0, 0), (1, 0), (0, 1), (1, 1))
OFFS = (0, 1, 3, 2)
ROWS = 144


def from_offset(value, axis, step, n=4):
    return lax.ppermute(value, axis, [((k + step) % n, k) for k in range(n)])


def others(value, axis):
    parts = []
    for i in OFFS[1:]:
        parts.append(from_offset(value, axis, i))
    return parts


def swapped(value):
    return lax.ppermute(value, "core", [(0, 1), (1, 0)])


def features_of(values):
    wide = values.astype(jnp.float32)
    return jnp.where(wide > 0.0, wide + 1.0, jnp.exp(wide)).astype(jnp.bfloat16)


def sums_kernel(where, keys_ref, values_ref, keep_ref, give_ref):
    x = where[2]
    half, seq = pl.program_id(0), pl.program_id(1)
    keys = jnp.swapaxes(features_of(keys_ref[0]), 0, 1)
    values = jnp.swapaxes(values_ref[0], 0, 1)

    def store(out_ref):
        for h in range(8):
            slot = lax.rem(h // 2 - x + 4, 4)
            state = lax.dot_general(
                values[h], keys[h], (((0,), (0,)), ((), ())), preferred_element_type=jnp.float32
            )
            mass = jnp.sum(keys[h].astype(jnp.float32), 0, keepdims=True)
            out_ref[slot, h % 2, seq, :SIZE] = state.astype(jnp.bfloat16)
            out_ref[slot, h % 2, seq, SIZE:] = jnp.broadcast_to(mass, (16, SIZE)).astype(
                jnp.bfloat16
            )

    @pl.when(half == 0)
    def _():
        store(give_ref)

    @pl.when(half == 1)
    def _():
        store(keep_ref)


def partial_sums(where, offered, contents):
    block = pl.BlockSpec(
        (1, 256, 8, SIZE), lambda g, s, where: (s, 0, lax.rem(where[3] + 1 + g, 2), 0)
    )
    whole = pl.BlockSpec((4, 2, 2, ROWS, SIZE), lambda g, s, where: (0, 0, 0, 0, 0))
    out = jax.ShapeDtypeStruct((4, 2, 2, ROWS, SIZE), jnp.bfloat16)
    return pl.pallas_call(
        sums_kernel,
        out_shape=(out, out),
        grid_spec=pltpu.PrefetchScalarGridSpec(
            num_scalar_prefetch=1,
            grid=(2, 2),
            in_specs=[block, block],
            out_specs=(whole, whole),
        ),
        cost_estimate=pl.CostEstimate(flops=5 << 30, bytes_accessed=5 << 20, transcendentals=0),
        compiler_params=pltpu.CompilerParams(vmem_limit_bytes=24 << 20),
        name="sums",
    )(where, offered, contents)


def pack_kernel(weight, out_ref, half_ref, sems):
    x, base = lax.axis_index("x"), lax.axis_index("core") * HALF
    copies = []
    for n, (r, c) in enumerate(BLOCKS):
        rows = 64 if n < NY else 16
        first = r * 64 if n < NY else pl.multiple_of(r * 64 + x * 16, 16)
        at = n * 64 if n < NY else NY * 64 + (n - NY) * 16
        copies.append(
            pltpu.make_async_copy(
                weight.at[pl.ds(first, rows), pl.ds(pl.multiple_of(base + c * 512, 512), 512)],
                out_ref.at[pl.ds(at, rows)],
                sems.at[n],
            )
        )
    columns = pl.ds(pl.multiple_of(base, HALF), HALF)
    copies.append(pltpu.make_async_copy(weight.at[:, columns], half_ref, sems.at[4]))
    for copy in copies:
        copy.start()
    for copy in copies:
        copy.wait()


def pack(weight):
    vmem = pl.BlockSpec(memory_space=pltpu.VMEM)
    return pl.pallas_call(
        pack_kernel,
        out_shape=(
            jax.ShapeDtypeStruct((NY * 64 + NX * 16, 512), jnp.bfloat16),
            jax.ShapeDtypeStruct((128, HALF), jnp.bfloat16),
        ),
        in_specs=[pl.BlockSpec(memory_space=pltpu.HBM)],
        out_specs=(vmem, vmem),
        scratch_shapes=[pltpu.SemaphoreType.DMA((5,))],
        name="pack",
    )(weight)


def queries_kernel(asked_ref, gates_ref, features_ref, factors_ref):
    features = jnp.swapaxes(features_of(asked_ref[0]), 0, 1)
    gates = gates_ref[0].astype(jnp.float32)
    factors = jnp.swapaxes((64.0 / (1.0 + jnp.exp(-gates))).astype(jnp.bfloat16), 0, 1)
    features_ref[:, 0] = features
    factors_ref[:, 0] = factors


def query_features(asked_for, gate_rows):
    block = pl.BlockSpec((1, 256, 8, SIZE), lambda s, g: (s, 0, g, 0))
    out_block = pl.BlockSpec((8, 1, 256, SIZE), lambda s, g: (g, s, 0, 0))
    out = jax.ShapeDtypeStruct((HEADS, 2, 256, SIZE), jnp.bfloat16)
    return pl.pallas_call(
        queries_kernel,
        out_shape=(out, out),
        grid=(2, 2),
        in_specs=[block, block],
        out_specs=(out_block, out_block),
        cost_estimate=pl.CostEstimate(flops=5 << 30, bytes_accessed=8 << 20, transcendentals=0),
        compiler_params=pltpu.CompilerParams(vmem_limit_bytes=24 << 20),
        name="queries",
    )(asked_for, gate_rows)


N_CHUNKS = 22


def project_kernel(where, weight, features_ref, factors_ref, *rest):
    states, chunks = rest[:8], rest[8 : 8 + N_CHUNKS]
    out_ref, held, mixed, done, sems = rest[8 + N_CHUNKS :]
    zh, y, x, core = where[0], where[1], where[2], where[3]
    copies = ([], [], [], [])
    for k in range(2):
        base = (core if k == 0 else 1 - core) * HALF
        by_y, by_x = chunks[6 + k * 8 : 10 + k * 8], chunks[10 + k * 8 : 14 + k * 8]

        def copy(source, row, rows, c):
            copies[k * 2 + c].append((source, row, rows))

        for j in range(4):
            for z in range(4):
                shard = (lax.rem(zh + OFFS[z], 4) * 4 + lax.rem(y + OFFS[j], 4)) * 128
                if z == 0:
                    near, first = (chunks[k * 3 + j - 1], 0) if j else (weight, base)
                    for c in range(2):
                        columns = pl.ds(pl.multiple_of(first + c * 512, 512), 512)
                        copy(near.at[:, columns], shard, 128, c)
                    continue
                for n, (r, c) in enumerate(BLOCKS):
                    row = shard + r * 64
                    if n < NY:
                        copy(by_y[j].at[z - 1, pl.ds(n * 64, 64)], row, 64, c)
                        continue
                    for i in range(4):
                        copy(
                            by_x[i].at[j, z - 1, pl.ds((n - NY) * 16, 16)],
                            row + lax.rem(x + OFFS[i], 4) * 16,
                            16,
                            c,
                        )
    for p in range(8):
        half = core if p < 4 else 1 - core
        for h in range(2):
            head = half * 8 + lax.rem(x + OFFS[p % 4], 4) * 2 + h
            for s in range(2):
                state = states[p][h, s]
                both = jnp.concatenate(
                    [state[:SIZE], jnp.broadcast_to(state[SIZE : SIZE + 1], (SIZE, SIZE))], 0
                )
                read = lax.dot_general(
                    features_ref[head, s],
                    both,
                    (((1,), (1,)), ((), ())),
                    preferred_element_type=jnp.float32,
                )
                scaled = read[:, :SIZE] / (read[:, SIZE:] + 4.096)
                gated = scaled * factors_ref[head, s].astype(jnp.float32)
                mixed[pl.ds(s * 256, 256), pl.ds(pl.multiple_of(head * SIZE, SIZE), SIZE)] = (
                    gated.astype(jnp.bfloat16)
                )
    out_copies = []
    for n, group in enumerate(copies):
        for source, row, rows in group:
            held[n, pl.ds(pl.multiple_of(row, rows), rows)] = source[...]
        done[n] = jnp.dot(mixed[...], held[n], preferred_element_type=jnp.float32).astype(
            jnp.bfloat16
        )
        column = (core if n < 2 else 1 - core) * HALF + n % 2 * 512
        out_copies.append(
            pltpu.make_async_copy(
                done.at[n], out_ref.at[:, pl.ds(pl.multiple_of(column, 512), 512)], sems.at[n]
            )
        )
        out_copies[n].start()
    for one in out_copies:
        one.wait()


def project(where, weight, features, factors, states, chunks):
    vmem = pl.BlockSpec(memory_space=pltpu.VMEM)
    return pl.pallas_call(
        project_kernel,
        out_shape=jax.ShapeDtypeStruct((512, WIDTH), jnp.bfloat16),
        in_specs=[pl.BlockSpec(memory_space=pltpu.SMEM)] + [vmem] * (11 + N_CHUNKS),
        out_specs=pl.BlockSpec(memory_space=pltpu.HBM),
        scratch_shapes=[
            pltpu.VMEM((4, WIDTH, 512), jnp.bfloat16),
            pltpu.VMEM((512, WIDTH), jnp.bfloat16),
            pltpu.VMEM((4, 512, 512), jnp.bfloat16),
            pltpu.SemaphoreType.DMA((4,)),
        ],
        cost_estimate=pl.CostEstimate(
            flops=2 * 512 * WIDTH * WIDTH, bytes_accessed=16 << 20, transcendentals=0
        ),
        compiler_params=pltpu.CompilerParams(vmem_limit_bytes=40 << 20),
        name="project",
    )(where, weight, features, factors, *states, *chunks)


def add_up(parts):
    return sum(part.astype(jnp.float32) for part in parts).astype(jnp.bfloat16)


def reduced(keep, give):
    taken = swapped(give)
    mine = [add_up((keep[i], taken[i])) for i in range(4)]
    parts = [mine[0]]
    for i in OFFS[1:]:
        parts.append(from_offset(mine[4 - i], "x", i))
    two = add_up(parts)
    other = lax.ppermute(two, "zl", [(0, 1), (1, 0)])
    two = add_up((two, other))
    pieces = [two] + others(two, "x")
    return pieces + [swapped(piece) for piece in pieces]


def local(asked_for, offered, contents, gate_rows, out_weight):
    place = [lax.axis_index(a) for a in ("zh", "y", "x", "core")]
    where = jnp.stack(place).astype(jnp.int32)
    hbm = lambda value: pltpu.with_memory_space_constraint(value, pltpu.HBM)
    packed, half = pack(hbm(out_weight))
    far = others(packed, "zh")
    own = others(half, "y")
    keep, give = partial_sums(where, hbm(offered), hbm(contents))
    far_y = jnp.stack([part[: NY * 64] for part in far])
    far_x = jnp.stack([part[NY * 64 :] for part in far])
    by_y = [far_y] + others(far_y, "y")
    set_x = jnp.stack([far_x] + others(far_x, "y"))
    chunks = by_y + [set_x] + others(set_x, "x")
    own += [swapped(part) for part in own]
    early = swapped(far_y)
    chunks = own + chunks + [early] + [swapped(chunk) for chunk in chunks[1:]]
    states = reduced(keep, give)
    features, factors = query_features(hbm(asked_for), hbm(gate_rows))
    return project(where, out_weight, features, factors, states, chunks).reshape(2, 256, WIDTH)


def solution(mesh):
    finer = Mesh(mesh.devices.reshape(4, 4, 2, 4, 2), BATCH + CTX)
    rows = P(BATCH, CTX, None, None)
    return jax.shard_map(
        local,
        mesh=finer,
        in_specs=(rows, rows, rows, rows, P(BATCH, None)),
        out_specs=P(BATCH, CTX, None),
        check_vma=False,
    )
```
